256 devices in a mesh: dp: 16 (over y, x_hi, core), tensor: 16 (over x_lo, z).
Axes of the slice: x: 4 (x_hi: 2, x_lo: 2; x = x_hi * 2 + x_lo), y: 4, z: 8, core: 2. Of those that a mesh axis runs over, the one named last changes fastest.
Arguments:
- h_values: bfloat16 [12288, 16384], P(('dp', 'tensor')), may hold values from -448 to 448
- h_scales: bfloat16 [12288, 128], P(('dp', 'tensor')), may hold values from 0.00049972534 to 0.0099487305
- dy_values: bfloat16 [12288, 4096], P(('dp', 'tensor')), may hold values from -448 to 448
- dy_scales: bfloat16 [12288, 32], P(('dp', 'tensor')), may hold values from 1.9907951e-05 to 0.00039863586
Outputs:
- grad_down: bfloat16 [4096, 16384], P('dp', 'tensor')
The draws below stay inside these ranges and needn't reach their ends.
All inputs are finite; a program needn't handle non-finite values.
Results may differ from the reference program's by a relative error of at most 0.02.
Values may be sent and summed in bfloat16 or wider, within the bound.
A program may use at most 192 MiB of HBM per device.

```python
import math
import jax
import jax.numpy as jnp
from jax import lax

D = 4096
FF = 16384
QBLOCK = 128
GROUP_TOK = 768
TOKENS = 12288
N_DP = 16


def steps_of(rng, shape, cuts, smallest, top_value):
    def one(dim, blocks):
        heights = jax.random.uniform(jax.random.fold_in(jax.random.fold_in(rng, 6), dim), (blocks,), jnp.float32, smallest / len(cuts), top_value / len(cuts))
        return jnp.repeat(jnp.exp(heights), shape[dim] // blocks).reshape((-1,) + (1,) * (len(shape) - dim - 1))

    level = one(*cuts[0])
    for cut in cuts[1:]:
        level = level * one(*cut)
    return level


def setup_inputs(seed: int = 0) -> dict:
    key_of = jax.random.split(jax.random.key(seed), 5)
    return {
        "h_values": jnp.clip(jax.random.uniform(key_of[0], (TOKENS, FF), jnp.float32, -448.0, 448.0) * steps_of(key_of[0], (TOKENS, FF), ((0, 256),), -0.4, 0.0), -448.0, 448.0).astype(jnp.bfloat16),
        "h_scales": jnp.clip(jnp.exp(math.log(0.0099487305) - 2.9911416 * jax.random.uniform(key_of[1], (TOKENS, FF // QBLOCK), jnp.float32) ** steps_of(key_of[1], (TOKENS, FF // QBLOCK), ((0, 256),), -0.2, 0.2)), 0.00049972534, 0.0099487305).astype(jnp.bfloat16),
        "dy_values": jnp.clip(jax.random.uniform(key_of[2], (TOKENS, D), jnp.float32, -448.0, 448.0) * steps_of(key_of[2], (TOKENS, D), ((0, 256),), -0.4, 0.0), -448.0, 448.0).astype(jnp.bfloat16),
        "dy_scales": jnp.clip(jnp.exp(math.log(0.00039863586) - 2.9969292 * jax.random.uniform(key_of[3], (TOKENS, D // QBLOCK), jnp.float32) ** steps_of(key_of[3], (TOKENS, D // QBLOCK), ((0, 256),), -0.2, 0.2)), 1.990795135498047e-05, 0.00039863586).astype(jnp.bfloat16),
    }


def dequantize(values, scales):
    row_count, col_count = values.shape
    block_total = scales.shape[1]
    widened = values.astype(jnp.float32).reshape(row_count, block_total, col_count // block_total)
    widened = widened * scales.astype(jnp.float32)[:, :, None]
    return widened.reshape(row_count, col_count)


def requantize(field):
    row_count, col_count = field.shape
    blocked = field.reshape(row_count // QBLOCK, QBLOCK, col_count)
    largest = jnp.max(jnp.abs(blocked), axis=1)
    column_scale = ((largest + 1e-6) / 448.0).astype(jnp.bfloat16)
    quantized = (blocked / column_scale.astype(jnp.float32)[:, None, :]).astype(jnp.bfloat16)
    return quantized.reshape(row_count, col_count), column_scale


def group_product(grad_q, grad_scale, hidden_q, hidden_scale):
    block_count = grad_q.shape[0] // QBLOCK
    summed = jnp.zeros((grad_q.shape[1], hidden_q.shape[1]), jnp.float32)
    for block_index in range(block_count):
        grad_block = grad_q[block_index * QBLOCK:(block_index + 1) * QBLOCK].astype(jnp.float32)
        hidden_block = hidden_q[block_index * QBLOCK:(block_index + 1) * QBLOCK].astype(jnp.float32)
        product = jnp.dot(grad_block.T, hidden_block, precision=lax.Precision.HIGHEST, preferred_element_type=jnp.float32)
        row_factor = grad_scale[block_index].astype(jnp.float32)[:, None]
        col_factor = hidden_scale[block_index].astype(jnp.float32)[None, :]
        summed = summed + product * row_factor * col_factor
    return summed


def reference(h_values, h_scales, dy_values, dy_scales):
    hidden_q, hidden_scale = requantize(dequantize(h_values, h_scales))
    grad_q, grad_scale = requantize(dequantize(dy_values, dy_scales))
    block_count = GROUP_TOK // QBLOCK

    def one_group(summed, group_index):
        row_begin = (group_index * GROUP_TOK).astype(jnp.int32)
        block_begin = (group_index * block_count).astype(jnp.int32)
        partial_value = group_product(
            lax.dynamic_slice_in_dim(grad_q, row_begin, GROUP_TOK, 0),
            lax.dynamic_slice_in_dim(grad_scale, block_begin, block_count, 0),
            lax.dynamic_slice_in_dim(hidden_q, row_begin, GROUP_TOK, 0),
            lax.dynamic_slice_in_dim(hidden_scale, block_begin, block_count, 0))
        rounded = lax.optimization_barrier(partial_value.astype(jnp.bfloat16)).astype(jnp.float32)
        return summed + rounded, None

    result = lax.scan(one_group, jnp.zeros((D, FF), jnp.float32), jnp.arange(N_DP, dtype=jnp.int32))
    return result[0].astype(jnp.bfloat16)
```

```python
import jax
import jax.numpy as jnp
from jax import lax
from jax.experimental import pallas as pl
from jax.experimental.pallas import tpu as pltpu
from jax.sharding import PartitionSpec as P

QBLOCK = 128
MESH = pl.DeviceIdType.MESH
XN, YN, ZN = 4, 4, 8
TOK = 48
LINE = ZN * TOK
KTOK = XN * LINE
ROWS = 1024
HALF = ROWS // 2
COLS = 2048
NCH = 4
W = COLS // NCH
F32, BF16 = jnp.float32, jnp.bfloat16


def requantize(block):
    largest = jnp.max(jnp.abs(block), axis=0, keepdims=True)
    scale = ((largest + 1e-6) / 448.0).astype(BF16).astype(F32)
    quantized = (block * (1.0 / scale)).astype(BF16).astype(F32)
    return quantized * scale


def kernel(hv, hs, dv, ds, out,
           dyp, gat, hsend, hz, hx, gt, px, pr, po,
           sp, sm, rp, rm, cp, cm, qp, qm, fb, fr,
           hss, hrs, dxs, dxr, dzs, dzr, xss, xrs, xfs, xfr, cs, cr, ys, yr, fs, frs):
    dp, t = lax.axis_index("dp"), lax.axis_index("tensor")
    c, xh, y = dp % 2, (dp // 2) % 2, dp // 4
    xl, z = t // 8, t % 8
    x = xh * 2 + xl

    def dev(x_=None, y_=None, z_=None, c_=None):
        x_ = x if x_ is None else x_
        y_ = y if y_ is None else y_
        z_ = z if z_ is None else z_
        c_ = c if c_ is None else c_
        return ((y_ * 2 + x_ // 2) * 2 + c_, (x_ % 2) * 8 + z_)

    def send(src, dst, ssem, rsem, to):
        return pltpu.make_async_remote_copy(
            src_ref=src, dst_ref=dst, send_sem=ssem, recv_sem=rsem, device_id=to, device_id_type=MESH)

    def zrow(zs):
        return pl.ds(pl.multiple_of(zs * TOK, 16), TOK)

    def xrow(xs, lo=0, n=LINE):
        return pl.ds(pl.multiple_of(xs * LINE + lo, 16), n)

    barrier = pltpu.get_barrier_semaphore()
    peers = ([dev(x_=(x + d) % XN) for d in range(1, XN)] + [dev(y_=(y + d) % YN) for d in (1, 3)]
             + [dev(z_=(z + d) % ZN) for d in range(1, ZN)] + [dev(c_=1 - c)])
    for peer in peers:
        pl.semaphore_signal(barrier, inc=1, device_id=peer, device_id_type=MESH)

    for j in range(32):
        y_, a_, c_, b_ = j // 8, (j // 4) % 2, (j // 2) % 2, j % 2
        q = c_ * YN + y_
        val = dv[:, j * 128:(j + 1) * 128].astype(F32) * ds[:, j:j + 1].astype(F32)
        dyp[a_ * 2 + b_, :, q * 128:(q + 1) * 128] = val.astype(BF16)
    gat[x, zrow(z), :] = dyp[x]

    pl.semaphore_wait(barrier, len(peers))

    dx = []
    for d in range(1, XN):
        to = (x + d) % XN
        cpy = send(dyp.at[to], gat.at[x, zrow(z)], dxs.at[d - 1], dxr.at[d - 1], dev(x_=to))
        cpy.start()
        dx.append(cpy)

    hcp = []
    blocks = W // 128
    for k in range(NCH):
        for zz in range(ZN):
            for i in range(blocks):
                col = k * W + i * 128
                j = ((col // 1024) * 8 + zz) * 8 + (col % 1024) // 128
                val = hv[:, j * 128:(j + 1) * 128].astype(F32) * hs[:, j:j + 1].astype(F32)
                hsend[k, zz, :, i * 128:(i + 1) * 128] = val.astype(BF16)
        row = []
        for n, d in enumerate((1, 7, 2, 6, 3, 5, 4)):
            to = (z + d) % ZN
            cpy = send(hsend.at[k, to], hz.at[k, zrow(z)], hss.at[k, n], hrs.at[k, n], dev(z_=to))
            cpy.start()
            row.append(cpy)
        hcp.append(row)
        hz[k, zrow(z), :] = hsend[k, z]

    zu, zd = dev(z_=(z + 1) % ZN), dev(z_=(z + 7) % ZN)

    def ring(s):
        su, sd = (z + 8 - s) % ZN, (z + s) % ZN
        if s < 3:
            up, dn = gat.at[:, zrow(su)], gat.at[:, zrow(sd)]
        else:
            up, dn = gat.at[0:2, zrow(su)], gat.at[2:4, zrow(sd)]
        return (send(up, up, dzs.at[0, s], dzr.at[0, s], zu), send(dn, dn, dzs.at[1, s], dzr.at[1, s], zd))

    rings = [ring(s) for s in range(4)]
    for cpy in dx:
        cpy.wait_recv()
    for cpy in rings[0]:
        cpy.start()

    xu, xd = dev(x_=(x + 1) % XN), dev(x_=(x + 3) % XN)
    xup, xdn = (x + 3) % XN, (x + 1) % XN
    xcp, fcp = [], []

    def forward(k):
        for cpy in xcp[k]:
            cpy.wait_recv()
        up, dn = hx.at[k, xrow(xup, 0, LINE // 2)], hx.at[k, xrow(xdn, LINE // 2, LINE // 2)]
        pair = (send(up, up, xfs.at[k, 0], xfr.at[k, 0], xu), send(dn, dn, xfs.at[k, 1], xfr.at[k, 1], xd))
        for cpy in pair:
            cpy.start()
        fcp.append(pair)

    for k in range(NCH):
        for cpy in hcp[k]:
            cpy.wait_recv()

        @pl.loop(0, W // 128)
        def _(i):
            lanes = pl.ds(pl.multiple_of(i * 128, 128), 128)
            for b in range(LINE // QBLOCK):
                val = requantize(hz[k, b * QBLOCK:(b + 1) * QBLOCK, lanes].astype(F32))
                hx[k, xrow(x, b * QBLOCK, QBLOCK), lanes] = val.astype(BF16)

        mine = hx.at[k, xrow(x)]
        pair = (send(mine, mine, xss.at[k, 0], xrs.at[k, 0], xu), send(mine, mine, xss.at[k, 1], xrs.at[k, 1], xd))
        for cpy in pair:
            cpy.start()
        xcp.append(pair)
        if k:
            forward(k - 1)
    forward(NCH - 1)

    for s in range(4):
        for cpy in rings[s]:
            cpy.wait_recv()
        if s < 3:
            for cpy in rings[s + 1]:
                cpy.start()

    for b in range(KTOK // QBLOCK):
        xs, bb = b // 3, b % 3

        @pl.loop(0, ROWS // 128)
        def _(i):
            at = pl.ds(pl.multiple_of(i * 128, 128), 128)
            val = requantize(gat[xs, bb * QBLOCK:(bb + 1) * QBLOCK, at].astype(F32))
            gt[at, b * QBLOCK:(b + 1) * QBLOCK] = val.T.astype(BF16)

    partner = dev(c_=1 - c)
    yu, yd = dev(y_=(y + 1) % YN), dev(y_=(y + 3) % YN)
    core_cp, ring_cp, tail_cp = [], [], []

    def product(k):
        for cpy in fcp[k]:
            cpy.wait_recv()

        @pl.loop(0, 2)
        def _(i):
            rows = pl.ds(pl.multiple_of((1 - c) * HALF + i * 256, 256), 256)
            at = pl.ds(pl.multiple_of(i * 256, 256), 256)
            px[k, at, :] = jnp.dot(gt[rows, :], hx[k], preferred_element_type=F32).astype(BF16)

        cpy = send(px.at[k], pr.at[k], cs.at[k], cr.at[k], partner)
        cpy.start()
        core_cp.append(cpy)

        @pl.loop(0, 2)
        def _(i):
            rows = pl.ds(pl.multiple_of(c * HALF + i * 256, 256), 256)
            at = pl.ds(pl.multiple_of(i * 256, 256), 256)
            po[k, at, :] = jnp.dot(gt[rows, :], hx[k], preferred_element_type=F32)

    def part(k, yy, lo):
        return po[k, pl.ds(pl.multiple_of(yy * 128 + lo, 64), 64), :]

    y1, y2, y3 = (y + 1) % YN, (y + 2) % YN, (y + 3) % YN

    def reduce_first(k):
        core_cp[k].wait_recv()
        po[k] = po[k] + pr[k].astype(F32)
        sp[k, 0] = part(k, y2, 0).astype(BF16)
        sp[k, 1] = part(k, y1, 64).astype(BF16)
        sm[k, 0] = part(k, y2, 64).astype(BF16)
        sm[k, 1] = part(k, y3, 0).astype(BF16)
        pair = (send(sp.at[k], rp.at[k], ys.at[k, 0], yr.at[k, 0], yu),
                send(sm.at[k], rm.at[k], ys.at[k, 1], yr.at[k, 1], yd))
        for cpy in pair:
            cpy.start()
        ring_cp.append(pair)

    def reduce_second(k):
        for cpy in ring_cp[k]:
            cpy.wait_recv()
        cp[k] = (part(k, y1, 0) + rp[k, 0].astype(F32)).astype(BF16)
        cm[k] = (part(k, y3, 64) + rm[k, 0].astype(F32)).astype(BF16)
        pair = (send(cp.at[k], qp.at[k], ys.at[k, 2], yr.at[k, 2], yu),
                send(cm.at[k], qm.at[k], ys.at[k, 3], yr.at[k, 3], yd))
        for cpy in pair:
            cpy.start()
        tail_cp.append(pair)

    across = dev(x_=xh * 2 + 1 - xl)
    per = NCH // 2

    def swap(j, k):
        return send(fb.at[k], fr.at[j], fs.at[j], frs.at[j], across)

    def finish(k):
        for cpy in tail_cp[k]:
            cpy.wait_recv()
        fb[k, 0:64] = (part(k, y, 0) + qp[k].astype(F32) + rm[k, 1].astype(F32)).astype(BF16)
        fb[k, 64:128] = (part(k, y, 64) + qm[k].astype(F32) + rp[k, 1].astype(F32)).astype(BF16)

        @pl.when(xl != k // per)
        def _():
            swap(k % per, k).start()

    for k in range(NCH + 3):
        if k < NCH:
            product(k)
        if 0 <= k - 1 < NCH:
            reduce_first(k - 1)
        if 0 <= k - 2 < NCH:
            reduce_second(k - 2)
        if 0 <= k - 3 < NCH:
            finish(k - 3)

    mine_rows = pl.ds(pl.multiple_of(xl * 128, 128), 128)
    other_rows = pl.ds(pl.multiple_of((1 - xl) * 128, 128), 128)
    for j in range(per):
        out[mine_rows, j * W:(j + 1) * W] = fb[xl * per + j]
    for j in range(per):
        swap(j, (1 - xl) * per + j).wait()
        out[other_rows, j * W:(j + 1) * W] = fr[j]

    for group in hcp + [dx] + rings + xcp + fcp + [core_cp] + ring_cp + tail_cp:
        for cpy in group:
            cpy.wait_send()


def shards(h_values, h_scales, dy_values, dy_scales):
    vmem = pl.BlockSpec(memory_space=pltpu.VMEM)
    dma = pltpu.SemaphoreType.DMA
    return pl.pallas_call(
        kernel,
        out_shape=jax.ShapeDtypeStruct((256, 1024), BF16),
        in_specs=[vmem] * 4,
        out_specs=vmem,
        scratch_shapes=[
            pltpu.VMEM((XN, TOK, ROWS), BF16),
            pltpu.VMEM((XN, LINE, ROWS), BF16),
            pltpu.VMEM((NCH, ZN, TOK, W), BF16),
            pltpu.VMEM((NCH, LINE, W), BF16),
            pltpu.VMEM((NCH, KTOK, W), BF16),
            pltpu.VMEM((ROWS, KTOK), BF16),
            pltpu.VMEM((NCH, HALF, W), BF16),
            pltpu.VMEM((NCH, HALF, W), BF16),
            pltpu.VMEM((NCH, HALF, W), F32),
            pltpu.VMEM((NCH, 2, 64, W), BF16),
            pltpu.VMEM((NCH, 2, 64, W), BF16),
            pltpu.VMEM((NCH, 2, 64, W), BF16),
            pltpu.VMEM((NCH, 2, 64, W), BF16),
            pltpu.VMEM((NCH, 64, W), BF16),
            pltpu.VMEM((NCH, 64, W), BF16),
            pltpu.VMEM((NCH, 64, W), BF16),
            pltpu.VMEM((NCH, 64, W), BF16),
            pltpu.VMEM((NCH, 128, W), BF16),
            pltpu.VMEM((NCH // 2, 128, W), BF16),
            dma((NCH, 7)), dma((NCH, 7)),
            dma((3,)), dma((3,)),
            dma((2, 4)), dma((2, 4)),
            dma((NCH, 2)), dma((NCH, 2)),
            dma((NCH, 2)), dma((NCH, 2)),
            dma((NCH,)), dma((NCH,)),
            dma((NCH, 4)), dma((NCH, 4)),
            dma((NCH // 2,)), dma((NCH // 2,)),
        ],
        compiler_params=pltpu.CompilerParams(
            collective_id=0, has_side_effects=True, vmem_limit_bytes=60 * 1024 * 1024),
    )(h_values, h_scales, dy_values, dy_scales)


def solution(mesh):
    placed = P(("dp", "tensor"), None)
    return jax.shard_map(
        shards, mesh=mesh, in_specs=(placed,) * 4, out_specs=P("dp", "tensor"), check_vma=False)
```

```python
import jax
import jax.numpy as jnp
from jax import lax
from jax.experimental import pallas as pl
from jax.experimental.pallas import tpu as pltpu
from jax.sharding import PartitionSpec as P

QBLOCK = 128
MESH = pl.DeviceIdType.MESH
XN, YN, ZN = 4, 4, 8
TOK = 48
LINE = ZN * TOK
KTOK = XN * LINE
HALF = 512
COLS = 2048
NCH = 8
W = COLS // NCH
F32, BF16 = jnp.float32, jnp.bfloat16
NT = (((1,), (1,)), ((), ()))
ORDER = (
    ("dy",), ("bar",), ("x0",), ("h", 0), ("h", 1), ("s", 0, 0), ("s", 1, 0), ("r", 0), ("r", 1), ("f", 0),
    ("s", 0, 1), ("h", 2), ("f", 1), ("s", 0, 2), ("h", 3), ("r", 2), ("s", 0, 3), ("s", 1, 1), ("f", 2), ("h", 4),
    ("r", 3), ("q", 0), ("P", 0, 0), ("P", 0, 1), ("P", 0, 2), ("s", 1, 2), ("f", 3), ("A", 0, 0), ("h", 5),
    ("A", 0, 1), ("A", 0, 2), ("B", 0, 0), ("P", 0, 3), ("r", 4), ("B", 0, 1), ("B", 0, 2), ("A", 0, 3),
    ("E", 0, 0), ("s", 1, 3), ("h", 6), ("E", 0, 1), ("E", 0, 2), ("B", 0, 3), ("h", 7), ("f", 4), ("r", 5),
    ("E", 0, 3), ("q", 1), ("P", 1, 0), ("P", 1, 1), ("P", 1, 2), ("P", 1, 3), ("P", 0, 4), ("f", 5), ("r", 6),
    ("A", 1, 0), ("A", 1, 1), ("P", 1, 4), ("A", 1, 2), ("A", 1, 3), ("A", 0, 4), ("A", 1, 4), ("B", 1, 0),
    ("r", 7), ("P", 0, 5), ("P", 1, 5), ("B", 1, 1), ("B", 1, 2), ("A", 0, 5), ("A", 1, 5), ("B", 1, 3), ("f", 6),
    ("B", 0, 4), ("B", 1, 4), ("E", 1, 0), ("E", 1, 1), ("f", 7), ("E", 1, 2), ("B", 0, 5), ("P", 0, 6),
    ("P", 1, 6), ("B", 1, 5), ("E", 1, 3), ("E", 0, 4), ("A", 0, 6), ("P", 0, 7), ("A", 1, 6), ("E", 1, 4),
    ("P", 1, 7), ("E", 0, 5), ("E", 1, 5), ("A", 0, 7), ("A", 1, 7), ("B", 0, 6), ("B", 1, 6), ("B", 0, 7),
    ("B", 1, 7), ("E", 0, 6), ("E", 1, 6), ("E", 0, 7), ("E", 1, 7), ("END",),
)


def requantize(block):
    largest = jnp.max(jnp.abs(block), axis=0, keepdims=True)
    scale = ((largest + 1e-6) / 448.0).astype(BF16).astype(F32)
    quantized = (block * (1.0 / scale)).astype(BF16).astype(F32)
    return (quantized * scale).astype(BF16)


def kernel(hv_hbm, hs_hbm, dv_hbm, ds_hbm, out,
           hv, hs, dv, ds, eye, dyp, gat, hsend, hz, hx, gt, px, pr, po,
           sp, sm, rp, rm, cp, cm, qp, qm, fb, fr,
           ld, hss, hrs, dxs, dxr, dzs, dzr, xss, xrs, xfs, xfr, cs, cr, ys, yr, fs, frs):
    dp, t = lax.axis_index("dp"), lax.axis_index("tensor")
    c, xh, y = dp % 2, (dp // 2) % 2, dp // 4
    xl, z = t // 8, t % 8
    x = xh * 2 + xl

    def dev(x_=None, y_=None, z_=None, c_=None):
        x_ = x if x_ is None else x_
        y_ = y if y_ is None else y_
        z_ = z if z_ is None else z_
        c_ = c if c_ is None else c_
        return ((y_ * 2 + x_ // 2) * 2 + c_, (x_ % 2) * 8 + z_)

    def send(src, dst, ssem, rsem, to):
        return pltpu.make_async_remote_copy(
            src_ref=src, dst_ref=dst, send_sem=ssem, recv_sem=rsem, device_id=to, device_id_type=MESH)

    def zrow(zs):
        return pl.ds(pl.multiple_of(zs * TOK, 16), TOK)

    def xrow(xs, lo=0, n=LINE):
        return pl.ds(pl.multiple_of(xs * LINE + lo, 16), n)

    barrier = pltpu.get_barrier_semaphore()
    peers = ([dev(x_=(x + d) % XN) for d in range(1, XN)] + [dev(y_=(y + d) % YN) for d in (1, 3)]
             + [dev(z_=(z + d) % ZN) for d in range(1, ZN)] + [dev(c_=1 - c)])
    for peer in peers:
        pl.semaphore_signal(barrier, inc=1, device_id=peer, device_id_type=MESH)

    loads = [pltpu.make_async_copy(a, b, ld.at[n])
             for n, (a, b) in enumerate(((hv_hbm, hv), (hs_hbm, hs), (dv_hbm, dv), (ds_hbm, ds)))]
    for cpy in loads:
        cpy.start()
    eye[...] = (lax.broadcasted_iota(jnp.int32, (256, 256), 0)
                == lax.broadcasted_iota(jnp.int32, (256, 256), 1)).astype(F32).astype(BF16)
    for cpy in loads:
        cpy.wait()

    zu, zd = dev(z_=(z + 1) % ZN), dev(z_=(z + 7) % ZN)
    xu, xd = dev(x_=(x + 1) % XN), dev(x_=(x + 3) % XN)
    yu, yd = dev(y_=(y + 1) % YN), dev(y_=(y + 3) % YN)
    partner, across = dev(c_=1 - c), dev(x_=xh * 2 + 1 - xl)
    xup, xdn = (x + 3) % XN, (x + 1) % XN
    y1, y2, y3 = (y + 1) % YN, (y + 2) % YN, (y + 3) % YN
    per = NCH // 2

    x_dy = [[send(dyp.at[h, (x + d) % XN], gat.at[h, x, zrow(z)], dxs.at[h, d - 1], dxr.at[h, d - 1],
                  dev(x_=(x + d) % XN)) for d in range(1, XN)] for h in range(2)]
    z_h = [[send(hsend.at[k, (z + d) % ZN], hz.at[k, zrow(z)], hss.at[k, n], hrs.at[k, n], dev(z_=(z + d) % ZN))
            for n, d in enumerate((1, 7, 2, 6, 3, 5, 4))] for k in range(NCH)]

    def ring(h, s):
        lo, hi = (slice(0, 2), slice(2, 4)) if s == 3 else (slice(None), slice(None))
        up, dn = gat.at[h, lo, zrow((z + 8 - s) % ZN)], gat.at[h, hi, zrow((z + s) % ZN)]
        return (send(up, up, dzs.at[h, 0, s], dzr.at[h, 0, s], zu), send(dn, dn, dzs.at[h, 1, s], dzr.at[h, 1, s], zd))

    z_dy = [[ring(h, s) for s in range(4)] for h in range(2)]

    def x_first(k):
        mine = hx.at[k, xrow(x)]
        return (send(mine, mine, xss.at[k, 0], xrs.at[k, 0], xu), send(mine, mine, xss.at[k, 1], xrs.at[k, 1], xd))

    def x_second(k):
        up, dn = hx.at[k, xrow(xup, 0, LINE // 2)], hx.at[k, xrow(xdn, LINE // 2, LINE // 2)]
        return (send(up, up, xfs.at[k, 0], xfr.at[k, 0], xu), send(dn, dn, xfs.at[k, 1], xfr.at[k, 1], xd))

    x_h = [x_first(k) for k in range(NCH)]
    x_f = [x_second(k) for k in range(NCH)]
    core = [send(px.at[k], pr.at[k], cs.at[k], cr.at[k], partner) for k in range(NCH)]
    y_a = [(send(sp.at[k], rp.at[k], ys.at[k, 0], yr.at[k, 0], yu),
            send(sm.at[k], rm.at[k], ys.at[k, 1], yr.at[k, 1], yd)) for k in range(NCH)]
    y_b = [(send(cp.at[k], qp.at[k], ys.at[k, 2], yr.at[k, 2], yu),
            send(cm.at[k], qm.at[k], ys.at[k, 3], yr.at[k, 3], yd)) for k in range(NCH)]

    def swap(j, k):
        return send(fb.at[k], fr.at[j], fs.at[j], frs.at[j], across)

    def start(group):
        for cpy in group:
            cpy.start()

    def arrive(group):
        for cpy in group:
            cpy.wait_recv()

    def dequantize_dy():
        for j in range(32):
            y_, a_, c_, b_ = j // 8, (j // 4) % 2, (j // 2) % 2, j % 2
            val = dv[:, j * 128:(j + 1) * 128].astype(F32) * scales[:, j:j + 1]
            dyp[c_, a_ * 2 + b_, :, y_ * 128:(y_ + 1) * 128] = val.astype(BF16)
        for h in range(2):
            gat[h, x, zrow(z), :] = dyp[h, x]

    def send_dy():
        for h in range(2):
            start(x_dy[h])

    def send_h(k):
        for zz in range(ZN):
            for i in range(W // 128):
                col = k * W + i * 128
                j = ((col // 1024) * 8 + zz) * 8 + (col % 1024) // 128
                val = hv[:, j * 128:(j + 1) * 128].astype(F32) * hs[:, j:j + 1].astype(F32)
                hsend[k, zz, :, i * 128:(i + 1) * 128] = val.astype(BF16)
        start(z_h[k])
        hz[k, zrow(z), :] = hsend[k, z]

    def ring_dy(h, s):
        arrive(z_dy[h][s - 1] if s else x_dy[h])
        start(z_dy[h][s])

    def requantize_h(k):
        arrive(z_h[k])

        @pl.loop(0, W // 128)
        def _(i):
            lanes = pl.ds(pl.multiple_of(i * 128, 128), 128)
            for b in range(LINE // QBLOCK):
                hx[k, xrow(x, b * QBLOCK, QBLOCK), lanes] = requantize(
                    hz[k, b * QBLOCK:(b + 1) * QBLOCK, lanes].astype(F32))

        start(x_h[k])

    def forward_h(k):
        arrive(x_h[k])
        start(x_f[k])

    def requantize_dy(h):
        arrive(z_dy[h][3])
        for b in range(KTOK // 256):

            @pl.loop(0, HALF // 256)
            def _(i):
                at = pl.ds(pl.multiple_of(i * 256, 256), 256)
                vals = [requantize(gat[h, n // 3, (n % 3) * QBLOCK:(n % 3 + 1) * QBLOCK, at].astype(F32))
                        for n in (2 * b, 2 * b + 1)]
                turned = lax.dot_general(eye[...], jnp.concatenate(vals, 0), NT, preferred_element_type=F32)
                gt[pl.ds(pl.multiple_of(h * HALF + i * 256, 256), 256), b * 256:(b + 1) * 256] = turned.astype(BF16)

    def product(h, k):
        arrived = [x_f[k]]
        for group in arrived:
            if h == first_half[k]:
                arrive(group)

        @pl.when(c != h)
        def _():
            px[k] = jnp.dot(gt[h * HALF:(h + 1) * HALF, :], hx[k], preferred_element_type=F32).astype(BF16)
            core[k].start()

        @pl.when(c == h)
        def _():
            po[k] = jnp.dot(gt[h * HALF:(h + 1) * HALF, :], hx[k], preferred_element_type=F32)

    def part(k, yy, lo):
        return po[k, pl.ds(pl.multiple_of(yy * 128 + lo, 64), 64), :]

    def reduce_first(h, k):
        @pl.when(c == h)
        def _():
            core[k].wait_recv()
            po[k] = po[k] + pr[k].astype(F32)
            sp[k, 0] = part(k, y2, 0).astype(BF16)
            sp[k, 1] = part(k, y1, 64).astype(BF16)
            sm[k, 0] = part(k, y2, 64).astype(BF16)
            sm[k, 1] = part(k, y3, 0).astype(BF16)
            start(y_a[k])

    def reduce_second(h, k):
        @pl.when(c == h)
        def _():
            arrive(y_a[k])
            cp[k] = (part(k, y1, 0) + rp[k, 0].astype(F32)).astype(BF16)
            cm[k] = (part(k, y3, 64) + rm[k, 0].astype(F32)).astype(BF16)
            start(y_b[k])

    def finish(h, k):
        @pl.when(c == h)
        def _():
            arrive(y_b[k])
            fb[k, 0:64] = (part(k, y, 0) + qp[k].astype(F32) + rm[k, 1].astype(F32)).astype(BF16)
            fb[k, 64:128] = (part(k, y, 64) + qm[k].astype(F32) + rp[k, 1].astype(F32)).astype(BF16)

            @pl.when(xl != k // per)
            def _():
                swap(k % per, k).start()

    def conclude():
        mine_rows = pl.ds(pl.multiple_of(xl * 128, 128), 128)
        other_rows = pl.ds(pl.multiple_of((1 - xl) * 128, 128), 128)
        for j in range(per):
            out[mine_rows, j * W:(j + 1) * W] = fb[xl * per + j]
        for j in range(per):
            swap(j, (1 - xl) * per + j).wait()
            out[other_rows, j * W:(j + 1) * W] = fr[j]
        for group in x_dy + z_h + z_dy[0] + z_dy[1] + x_h + x_f + [core] + y_a + y_b:
            for cpy in group:
                cpy.wait_send()

    scales = lax.dot_general(eye[0:TOK, 0:TOK], ds[...], NT, preferred_element_type=F32)
    first_half = {}
    for step in ORDER:
        if step[0] == "P":
            first_half.setdefault(step[2], step[1])
    steps = dict(dy=dequantize_dy, bar=lambda: pl.semaphore_wait(barrier, len(peers)), x0=send_dy, h=send_h,
                 s=ring_dy, r=requantize_h, f=forward_h, q=requantize_dy, P=product, A=reduce_first,
                 B=reduce_second, E=finish, END=conclude)
    for step in ORDER:
        steps[step[0]](*step[1:])


def shards(h_values, h_scales, dy_values, dy_scales):
    dma = pltpu.SemaphoreType.DMA
    anywhere = pl.BlockSpec(memory_space=pl.ANY)
    return pl.pallas_call(
        kernel,
        out_shape=jax.ShapeDtypeStruct((256, 1024), BF16),
        in_specs=[anywhere] * 4,
        out_specs=pl.BlockSpec(memory_space=pltpu.VMEM),
        scratch_shapes=[
            pltpu.VMEM((TOK, 16384), BF16),
            pltpu.VMEM((TOK, 128), BF16),
            pltpu.VMEM((TOK, 4096), BF16),
            pltpu.VMEM((32, TOK), BF16),
            pltpu.VMEM((256, 256), BF16),
            pltpu.VMEM((2, XN, TOK, HALF), BF16),
            pltpu.VMEM((2, XN, LINE, HALF), BF16),
            pltpu.VMEM((NCH, ZN, TOK, W), BF16),
            pltpu.VMEM((NCH, LINE, W), BF16),
            pltpu.VMEM((NCH, KTOK, W), BF16),
            pltpu.VMEM((2 * HALF, KTOK), BF16),
            pltpu.VMEM((NCH, HALF, W), BF16),
            pltpu.VMEM((NCH, HALF, W), BF16),
            pltpu.VMEM((NCH, HALF, W), F32),
            pltpu.VMEM((NCH, 2, 64, W), BF16),
            pltpu.VMEM((NCH, 2, 64, W), BF16),
            pltpu.VMEM((NCH, 2, 64, W), BF16),
            pltpu.VMEM((NCH, 2, 64, W), BF16),
            pltpu.VMEM((NCH, 64, W), BF16),
            pltpu.VMEM((NCH, 64, W), BF16),
            pltpu.VMEM((NCH, 64, W), BF16),
            pltpu.VMEM((NCH, 64, W), BF16),
            pltpu.VMEM((NCH, 128, W), BF16),
            pltpu.VMEM((NCH // 2, 128, W), BF16),
            dma((4,)),
            dma((NCH, 7)), dma((NCH, 7)),
            dma((2, 3)), dma((2, 3)),
            dma((2, 2, 4)), dma((2, 2, 4)),
            dma((NCH, 2)), dma((NCH, 2)),
            dma((NCH, 2)), dma((NCH, 2)),
            dma((NCH,)), dma((NCH,)),
            dma((NCH, 4)), dma((NCH, 4)),
            dma((NCH // 2,)), dma((NCH // 2,)),
        ],
        compiler_params=pltpu.CompilerParams(
            collective_id=0, has_side_effects=True, vmem_limit_bytes=60 * 1024 * 1024),
    )(h_values, h_scales, dy_values, dy_scales.T)


def solution(mesh):
    placed = P(("dp", "tensor"), None)
    return jax.shard_map(
        shards, mesh=mesh, in_specs=(placed,) * 4, out_specs=P("dp", "tensor"), check_vma=False)
```

```python
import jax
import jax.numpy as jnp
from jax import lax
from jax.experimental import pallas as pl
from jax.experimental.pallas import tpu as pltpu
from jax.sharding import PartitionSpec as P

QBLOCK = 128
MESH = pl.DeviceIdType.MESH
XN, YN, ZN = 4, 4, 8
TOK = 48
LINE = ZN * TOK
KTOK = XN * LINE
HALF = 512
COLS = 2048
WIDTHS = (128, 384, 512, 512, 256, 128, 128)
NCH = len(WIDTHS)
STARTS = tuple(sum(WIDTHS[:k]) for k in range(NCH))
OWNER = tuple(start // 1024 for start in STARTS)
F32, BF16 = jnp.float32, jnp.bfloat16
NT = (((1,), (1,)), ((), ()))
ORDER = (
    ("dy",), ("bar",), ("h", 1), ("x0",), ("h", 2), ("s", 0, 0), ("r", 1), ("h", 3), ("r", 2), ("f", 1),
    ("s", 0, 1), ("f", 2), ("s", 1, 0), ("s", 0, 2), ("r", 3), ("h", 0), ("s", 0, 3), ("s", 1, 1), ("r", 0),
    ("f", 3), ("h", 4), ("q", 0), ("s", 1, 2), ("f", 0), ("P", 0, 1), ("P", 0, 2), ("h", 5), ("P", 0, 3), ("r", 4),
    ("A", 0, 2), ("A", 0, 1), ("A", 0, 3), ("P", 0, 0), ("s", 1, 3), ("h", 6), ("A", 0, 0), ("B", 0, 2), ("r", 5),
    ("B", 0, 1), ("B", 0, 3), ("f", 4), ("q", 1), ("r", 6), ("f", 5), ("P", 1, 3), ("P", 1, 2), ("P", 0, 4),
    ("A", 1, 3), ("P", 1, 1), ("A", 1, 2), ("f", 6), ("P", 1, 4), ("A", 0, 4), ("P", 0, 5), ("B", 0, 0),
    ("A", 1, 1), ("P", 1, 0), ("A", 1, 4), ("P", 1, 5), ("B", 1, 3), ("P", 1, 6), ("A", 0, 5), ("B", 1, 2),
    ("P", 0, 6), ("A", 1, 5), ("B", 0, 4), ("A", 1, 6), ("A", 1, 0), ("E", 0, 3), ("A", 0, 6), ("E", 0, 2),
    ("B", 1, 4), ("B", 1, 1), ("E", 1, 3), ("E", 1, 2), ("E", 0, 1), ("B", 1, 5), ("B", 0, 5), ("B", 1, 0),
    ("B", 1, 6), ("B", 0, 6), ("E", 1, 4), ("E", 0, 4), ("E", 1, 1), ("E", 0, 0), ("E", 1, 5), ("E", 0, 5),
    ("E", 1, 0), ("E", 1, 6), ("E", 0, 6), ("END",),
)


def requantize(block):
    largest = jnp.max(jnp.abs(block), axis=0, keepdims=True)
    scale = ((largest + 1e-6) / 448.0).astype(BF16).astype(F32)
    quantized = (block * (1.0 / scale)).astype(BF16).astype(F32)
    return (quantized * scale).astype(BF16)


def kernel(hv_hbm, hs_hbm, dv_hbm, ds_hbm, out,
           hv, hs, dv, ds, eye, dyp, gat, hsend, hz, hx, gt, px, pr, po,
           sp, sm, rp, rm, cp, cm, qp, qm, fb, fr,
           ld, hss, hrs, dxs, dxr, dzs, dzr, xss, xrs, xfs, xfr, cs, cr, ys, yr, fs, frs):
    dp, t = lax.axis_index("dp"), lax.axis_index("tensor")
    c, xh, y = dp % 2, (dp // 2) % 2, dp // 4
    xl, z = t // 8, t % 8
    x = xh * 2 + xl

    def dev(x_=None, y_=None, z_=None, c_=None):
        x_ = x if x_ is None else x_
        y_ = y if y_ is None else y_
        z_ = z if z_ is None else z_
        c_ = c if c_ is None else c_
        return ((y_ * 2 + x_ // 2) * 2 + c_, (x_ % 2) * 8 + z_)

    def send(src, dst, ssem, rsem, to):
        return pltpu.make_async_remote_copy(
            src_ref=src, dst_ref=dst, send_sem=ssem, recv_sem=rsem, device_id=to, device_id_type=MESH)

    def zrow(zs):
        return pl.ds(pl.multiple_of(zs * TOK, 16), TOK)

    def xrow(xs, lo=0, n=LINE):
        return pl.ds(pl.multiple_of(xs * LINE + lo, 16), n)

    barrier = pltpu.get_barrier_semaphore()
    peers = ([dev(x_=(x + d) % XN) for d in range(1, XN)] + [dev(y_=(y + d) % YN) for d in (1, 3)]
             + [dev(z_=(z + d) % ZN) for d in range(1, ZN)] + [dev(c_=1 - c)])
    for peer in peers:
        pl.semaphore_signal(barrier, inc=1, device_id=peer, device_id_type=MESH)

    loads = [pltpu.make_async_copy(a, b, ld.at[n])
             for n, (a, b) in enumerate(((hv_hbm, hv), (hs_hbm, hs), (dv_hbm, dv), (ds_hbm, ds)))]
    for cpy in loads:
        cpy.start()
    eye[...] = (lax.broadcasted_iota(jnp.int32, (256, 256), 0)
                == lax.broadcasted_iota(jnp.int32, (256, 256), 1)).astype(F32).astype(BF16)
    for cpy in loads:
        cpy.wait()

    zu, zd = dev(z_=(z + 1) % ZN), dev(z_=(z + 7) % ZN)
    xu, xd = dev(x_=(x + 1) % XN), dev(x_=(x + 3) % XN)
    yu, yd = dev(y_=(y + 1) % YN), dev(y_=(y + 3) % YN)
    partner, across = dev(c_=1 - c), dev(x_=xh * 2 + 1 - xl)
    xup, xdn = (x + 3) % XN, (x + 1) % XN
    y1, y2, y3 = (y + 1) % YN, (y + 2) % YN, (y + 3) % YN

    x_dy = [[send(dyp.at[h, (x + d) % XN], gat.at[h, x, zrow(z)], dxs.at[h, d - 1], dxr.at[h, d - 1],
                  dev(x_=(x + d) % XN)) for d in range(1, XN)] for h in range(2)]
    z_h = [[send(hsend[k].at[(z + d) % ZN], hz[k].at[zrow(z)], hss.at[k, n], hrs.at[k, n], dev(z_=(z + d) % ZN))
            for n, d in enumerate((1, 7, 2, 6, 3, 5, 4))] for k in range(NCH)]

    def ring(h, s):
        lo, hi = (slice(0, 2), slice(2, 4)) if s == 3 else (slice(None), slice(None))
        up, dn = gat.at[h, lo, zrow((z + 8 - s) % ZN)], gat.at[h, hi, zrow((z + s) % ZN)]
        return (send(up, up, dzs.at[h, 0, s], dzr.at[h, 0, s], zu), send(dn, dn, dzs.at[h, 1, s], dzr.at[h, 1, s], zd))

    z_dy = [[ring(h, s) for s in range(4)] for h in range(2)]

    def x_first(k):
        mine = hx[k].at[xrow(x)]
        return (send(mine, mine, xss.at[k, 0], xrs.at[k, 0], xu), send(mine, mine, xss.at[k, 1], xrs.at[k, 1], xd))

    def x_second(k):
        up, dn = hx[k].at[xrow(xup, 0, LINE // 2)], hx[k].at[xrow(xdn, LINE // 2, LINE // 2)]
        return (send(up, up, xfs.at[k, 0], xfr.at[k, 0], xu), send(dn, dn, xfs.at[k, 1], xfr.at[k, 1], xd))

    x_h = [x_first(k) for k in range(NCH)]
    x_f = [x_second(k) for k in range(NCH)]
    core = [send(px[k], pr[k], cs.at[k], cr.at[k], partner) for k in range(NCH)]
    y_a = [(send(sp[k], rp[k], ys.at[k, 0], yr.at[k, 0], yu),
            send(sm[k], rm[k], ys.at[k, 1], yr.at[k, 1], yd)) for k in range(NCH)]
    y_b = [(send(cp[k], qp[k], ys.at[k, 2], yr.at[k, 2], yu),
            send(cm[k], qm[k], ys.at[k, 3], yr.at[k, 3], yd)) for k in range(NCH)]

    swap = [send(fb[k], fr[k], fs.at[k], frs.at[k], across) for k in range(NCH)]

    def start(group):
        for cpy in group:
            cpy.start()

    def arrive(group):
        for cpy in group:
            cpy.wait_recv()

    def dequantize_dy():
        for j in range(32):
            y_, a_, c_, b_ = j // 8, (j // 4) % 2, (j // 2) % 2, j % 2
            val = dv[:, j * 128:(j + 1) * 128].astype(F32) * scales[:, j:j + 1]
            dyp[c_, a_ * 2 + b_, :, y_ * 128:(y_ + 1) * 128] = val.astype(BF16)
        for h in range(2):
            gat[h, x, zrow(z), :] = dyp[h, x]

    def send_dy():
        for h in range(2):
            start(x_dy[h])

    def dequantize_h(k):
        for zz in range(ZN):
            for i in range(WIDTHS[k] // 128):
                col = STARTS[k] + i * 128
                j = ((col // 1024) * 8 + zz) * 8 + (col % 1024) // 128
                val = hv[:, j * 128:(j + 1) * 128].astype(F32) * hs[:, j:j + 1].astype(F32)
                hsend[k][zz, :, i * 128:(i + 1) * 128] = val.astype(BF16)

    def send_h(k):
        if k:
            dequantize_h(k)
        start(z_h[k])
        hz[k][zrow(z), :] = hsend[k][z]

    def ring_dy(h, s):
        arrive(z_dy[h][s - 1] if s else x_dy[h])
        start(z_dy[h][s])

    def requantize_h(k):
        arrive(z_h[k])

        @pl.loop(0, WIDTHS[k] // 128)
        def _(i):
            lanes = pl.ds(pl.multiple_of(i * 128, 128), 128)
            for b in range(LINE // QBLOCK):
                hx[k][xrow(x, b * QBLOCK, QBLOCK), lanes] = requantize(
                    hz[k][b * QBLOCK:(b + 1) * QBLOCK, lanes].astype(F32))

        start(x_h[k])

    def forward_h(k):
        arrive(x_h[k])
        start(x_f[k])

    def requantize_dy(h):
        arrive(z_dy[h][3])
        for b in range(KTOK // 256):

            @pl.loop(0, HALF // 256)
            def _(i):
                at = pl.ds(pl.multiple_of(i * 256, 256), 256)
                vals = [requantize(gat[h, n // 3, (n % 3) * QBLOCK:(n % 3 + 1) * QBLOCK, at].astype(F32))
                        for n in (2 * b, 2 * b + 1)]
                turned = lax.dot_general(eye[...], jnp.concatenate(vals, 0), NT, preferred_element_type=F32)
                gt[pl.ds(pl.multiple_of(h * HALF + i * 256, 256), 256), b * 256:(b + 1) * 256] = turned.astype(BF16)

    def product(h, k):
        if h == first_half[k]:
            arrive(x_f[k])

        @pl.when(c != h)
        def _():
            px[k][...] = jnp.dot(gt[h * HALF:(h + 1) * HALF, :], hx[k][...], preferred_element_type=F32).astype(BF16)
            core[k].start()

        @pl.when(c == h)
        def _():
            po[k][...] = jnp.dot(gt[h * HALF:(h + 1) * HALF, :], hx[k][...], preferred_element_type=F32)

    def part(k, yy, lo):
        return po[k][pl.ds(pl.multiple_of(yy * 128 + lo, 64), 64), :]

    def reduce_first(h, k):
        @pl.when(c == h)
        def _():
            core[k].wait_recv()
            po[k][...] = po[k][...] + pr[k][...].astype(F32)
            sp[k][0] = part(k, y2, 0).astype(BF16)
            sp[k][1] = part(k, y1, 64).astype(BF16)
            sm[k][0] = part(k, y2, 64).astype(BF16)
            sm[k][1] = part(k, y3, 0).astype(BF16)
            start(y_a[k])

    def reduce_second(h, k):
        @pl.when(c == h)
        def _():
            arrive(y_a[k])
            cp[k][...] = (part(k, y1, 0) + rp[k][0].astype(F32)).astype(BF16)
            cm[k][...] = (part(k, y3, 64) + rm[k][0].astype(F32)).astype(BF16)
            start(y_b[k])

    def finish(h, k):
        @pl.when(c == h)
        def _():
            arrive(y_b[k])
            low = (part(k, y, 0) + qp[k][...].astype(F32) + rm[k][1].astype(F32)).astype(BF16)
            high = (part(k, y, 64) + qm[k][...].astype(F32) + rp[k][1].astype(F32)).astype(BF16)

            @pl.when(xl == OWNER[k])
            def _():
                out[pl.ds(pl.multiple_of(xl * 128, 64), 64), columns(k)] = low
                out[pl.ds(pl.multiple_of(xl * 128 + 64, 64), 64), columns(k)] = high

            @pl.when(xl != OWNER[k])
            def _():
                fb[k][0:64] = low
                fb[k][64:128] = high
                swap[k].start()

    def columns(k):
        return slice(STARTS[k] % 1024, STARTS[k] % 1024 + WIDTHS[k])

    def conclude():
        for k in last_chunks:
            @pl.when(xl == OWNER[k])
            def _():
                swap[k].wait_recv()
                out[pl.ds(pl.multiple_of((1 - xl) * 128, 128), 128), columns(k)] = fr[k][...]

            @pl.when(xl != OWNER[k])
            def _():
                swap[k].wait_send()
        for group in x_dy + z_h + z_dy[0] + z_dy[1] + x_h + x_f:
            for cpy in group:
                cpy.wait_send()
        for k in range(NCH):
            for cpy in (core[k],) + y_a[k] + y_b[k]:
                cpy.wait_send()

    scales = lax.dot_general(eye[0:TOK, 0:TOK], ds[...], NT, preferred_element_type=F32)
    first_half, last_chunks = {}, []
    for step in ORDER:
        if step[0] == "P":
            first_half.setdefault(step[2], step[1])
        if step[0] == "E":
            last_chunks = [k for k in last_chunks if k != step[2]] + [step[2]]
    steps = dict(dy=dequantize_dy, bar=lambda: pl.semaphore_wait(barrier, len(peers)), x0=send_dy, h=send_h,
                 s=ring_dy, r=requantize_h, f=forward_h, q=requantize_dy, P=product, A=reduce_first,
                 B=reduce_second, E=finish, END=conclude)
    dequantize_h(0)
    for step in ORDER:
        steps[step[0]](*step[1:])


def shards(h_values, h_scales, dy_values, dy_scales):
    dma = pltpu.SemaphoreType.DMA
    anywhere = pl.BlockSpec(memory_space=pl.ANY)

    def chunks(shape, dtype=BF16):
        return [pltpu.VMEM(shape + (width,), dtype) for width in WIDTHS]

    return pl.pallas_call(
        kernel,
        out_shape=jax.ShapeDtypeStruct((256, 1024), BF16),
        in_specs=[anywhere] * 4,
        out_specs=pl.BlockSpec(memory_space=pltpu.VMEM),
        scratch_shapes=[
            pltpu.VMEM((TOK, 16384), BF16),
            pltpu.VMEM((TOK, 128), BF16),
            pltpu.VMEM((TOK, 4096), BF16),
            pltpu.VMEM((32, TOK), BF16),
            pltpu.VMEM((256, 256), BF16),
            pltpu.VMEM((2, XN, TOK, HALF), BF16),
            pltpu.VMEM((2, XN, LINE, HALF), BF16),
            chunks((ZN, TOK)),
            chunks((LINE,)),
            chunks((KTOK,)),
            pltpu.VMEM((2 * HALF, KTOK), BF16),
            chunks((HALF,)),
            chunks((HALF,)),
            chunks((HALF,), F32),
            chunks((2, 64)), chunks((2, 64)), chunks((2, 64)), chunks((2, 64)),
            chunks((64,)), chunks((64,)), chunks((64,)), chunks((64,)),
            chunks((128,)), chunks((128,)),
            dma((4,)),
            dma((NCH, 7)), dma((NCH, 7)),
            dma((2, 3)), dma((2, 3)),
            dma((2, 2, 4)), dma((2, 2, 4)),
            dma((NCH, 2)), dma((NCH, 2)),
            dma((NCH, 2)), dma((NCH, 2)),
            dma((NCH,)), dma((NCH,)),
            dma((NCH, 4)), dma((NCH, 4)),
            dma((NCH,)), dma((NCH,)),
        ],
        compiler_params=pltpu.CompilerParams(
            collective_id=0, has_side_effects=True, vmem_limit_bytes=60 * 1024 * 1024),
    )(h_values, h_scales, dy_values, dy_scales.T)


def solution(mesh):
    placed = P(("dp", "tensor"), None)
    return jax.shard_map(
        shards, mesh=mesh, in_specs=(placed,) * 4, out_specs=P("dp", "tensor"), check_vma=False)
```

```python
import jax
import jax.numpy as jnp
from jax import lax
from jax.experimental import pallas as pl
from jax.experimental.pallas import tpu as pltpu
from jax.sharding import PartitionSpec as P

QBLOCK = 128
MESH = pl.DeviceIdType.MESH
XN, YN, ZN = 4, 4, 8
TOK = 48
LINE = ZN * TOK
KTOK = XN * LINE
HALF = 512
COLS = 2048
WIDTHS = (128, 384, 512, 512, 256, 128, 128)
NCH = len(WIDTHS)
STARTS = tuple(sum(WIDTHS[:k]) for k in range(NCH))
OWNER = tuple(start // 1024 for start in STARTS)
F32, BF16 = jnp.float32, jnp.bfloat16
NT = (((1,), (1,)), ((), ()))
ORDER = (
    ("dy",), ("bar",), ("h", 0), ("x0",), ("h", 3), ("r", 0), ("s", 0, 0), ("h", 1), ("r", 3), ("h", 2),
    ("s", 0, 1), ("f", 0), ("f", 3), ("r", 1), ("s", 1, 0), ("s", 0, 2), ("r", 2), ("s", 1, 1), ("f", 1),
    ("s", 0, 3), ("s", 1, 2), ("f", 2), ("h", 4), ("q", 0), ("P", 0, 1), ("P", 0, 3), ("P", 0, 0), ("s", 1, 3),
    ("P", 0, 2), ("A", 0, 1), ("A", 0, 0), ("h", 6), ("h", 5), ("r", 4), ("A", 0, 3), ("A", 0, 2), ("q", 1),
    ("B", 0, 3), ("r", 6), ("P", 1, 1), ("P", 1, 0), ("B", 0, 2), ("f", 4), ("B", 0, 1), ("P", 1, 3), ("A", 1, 1),
    ("r", 5), ("P", 1, 2), ("A", 1, 3), ("f", 6), ("P", 0, 4), ("B", 1, 1), ("E", 0, 3), ("A", 1, 2), ("f", 5),
    ("P", 1, 4), ("B", 1, 3), ("A", 0, 4), ("A", 1, 0), ("P", 1, 6), ("P", 0, 6), ("A", 1, 4), ("B", 1, 2),
    ("P", 0, 5), ("P", 1, 5), ("E", 1, 1), ("A", 1, 6), ("A", 0, 6), ("E", 0, 2), ("A", 0, 5), ("A", 1, 5),
    ("B", 1, 4), ("E", 1, 3), ("E", 0, 1), ("B", 0, 4), ("B", 1, 6), ("B", 1, 0), ("B", 0, 0), ("B", 0, 6),
    ("B", 0, 5), ("E", 1, 2), ("B", 1, 5), ("E", 1, 4), ("E", 0, 4), ("E", 1, 6), ("E", 1, 0), ("E", 0, 0),
    ("E", 0, 6), ("E", 0, 5), ("E", 1, 5), ("END",),
)


def requantize(block):
    largest = jnp.max(jnp.abs(block), axis=0, keepdims=True)
    scale = ((largest + 1e-6) / 448.0).astype(BF16).astype(F32)
    quantized = (block * (1.0 / scale)).astype(BF16).astype(F32)
    return (quantized * scale).astype(BF16)


def kernel(hv_hbm, hs_hbm, dv_hbm, ds_hbm, out,
           hv, hs, dv, ds, eye, dyp, gat, hsend, hz, hx, gt, px, pr, po,
           sp, sm, rp, rm, cp, cm, qp, qm, fb, fr,
           ld, hss, hrs, dxs, dxr, dzs, dzr, xss, xrs, xfs, xfr, cs, cr, ys, yr, fs, frs, os):
    dp, t = lax.axis_index("dp"), lax.axis_index("tensor")
    c, xh, y = dp % 2, (dp // 2) % 2, dp // 4
    xl, z = t // 8, t % 8
    x = xh * 2 + xl

    def dev(x_=None, y_=None, z_=None, c_=None):
        x_ = x if x_ is None else x_
        y_ = y if y_ is None else y_
        z_ = z if z_ is None else z_
        c_ = c if c_ is None else c_
        return ((y_ * 2 + x_ // 2) * 2 + c_, (x_ % 2) * 8 + z_)

    def send(src, dst, ssem, rsem, to):
        return pltpu.make_async_remote_copy(
            src_ref=src, dst_ref=dst, send_sem=ssem, recv_sem=rsem, device_id=to, device_id_type=MESH)

    def zrow(zs):
        return pl.ds(pl.multiple_of(zs * TOK, 16), TOK)

    def xrow(xs, lo=0, n=LINE):
        return pl.ds(pl.multiple_of(xs * LINE + lo, 16), n)

    barrier = pltpu.get_barrier_semaphore()
    peers = ([dev(x_=(x + d) % XN) for d in range(1, XN)] + [dev(y_=(y + d) % YN) for d in (1, 3)]
             + [dev(z_=(z + d) % ZN) for d in range(1, ZN)] + [dev(c_=1 - c)])
    for peer in peers:
        pl.semaphore_signal(barrier, inc=1, device_id=peer, device_id_type=MESH)

    loads = [pltpu.make_async_copy(a, b, ld.at[n])
             for n, (a, b) in enumerate(((hv_hbm, hv), (hs_hbm, hs), (dv_hbm, dv), (ds_hbm, ds)))]
    for cpy in loads:
        cpy.start()
    eye[...] = (lax.broadcasted_iota(jnp.int32, (256, 256), 0)
                == lax.broadcasted_iota(jnp.int32, (256, 256), 1)).astype(F32).astype(BF16)
    for cpy in loads:
        cpy.wait()

    zu, zd = dev(z_=(z + 1) % ZN), dev(z_=(z + 7) % ZN)
    xu, xd = dev(x_=(x + 1) % XN), dev(x_=(x + 3) % XN)
    yu, yd = dev(y_=(y + 1) % YN), dev(y_=(y + 3) % YN)
    partner, across = dev(c_=1 - c), dev(x_=xh * 2 + 1 - xl)
    xup, xdn = (x + 3) % XN, (x + 1) % XN
    y1, y2, y3 = (y + 1) % YN, (y + 2) % YN, (y + 3) % YN

    x_dy = [[send(dyp.at[h, (x + d) % XN], gat.at[h, x, zrow(z)], dxs.at[h, d - 1], dxr.at[h, d - 1],
                  dev(x_=(x + d) % XN)) for d in range(1, XN)] for h in range(2)]
    z_h = [[send(hsend[k].at[(z + d) % ZN], hz[k].at[zrow(z)], hss.at[k, n], hrs.at[k, n], dev(z_=(z + d) % ZN))
            for n, d in enumerate((1, 7, 2, 6, 3, 5, 4))] for k in range(NCH)]

    def ring(h, s):
        lo, hi = (slice(0, 2), slice(2, 4)) if s == 3 else (slice(None), slice(None))
        up, dn = gat.at[h, lo, zrow((z + 8 - s) % ZN)], gat.at[h, hi, zrow((z + s) % ZN)]
        return (send(up, up, dzs.at[h, 0, s], dzr.at[h, 0, s], zu), send(dn, dn, dzs.at[h, 1, s], dzr.at[h, 1, s], zd))

    z_dy = [[ring(h, s) for s in range(4)] for h in range(2)]

    def x_first(k):
        mine = hx[k].at[xrow(x)]
        return (send(mine, mine, xss.at[k, 0], xrs.at[k, 0], xu), send(mine, mine, xss.at[k, 1], xrs.at[k, 1], xd))

    def x_second(k):
        up, dn = hx[k].at[xrow(xup, 0, LINE // 2)], hx[k].at[xrow(xdn, LINE // 2, LINE // 2)]
        return (send(up, up, xfs.at[k, 0], xfr.at[k, 0], xu), send(dn, dn, xfs.at[k, 1], xfr.at[k, 1], xd))

    x_h = [x_first(k) for k in range(NCH)]
    x_f = [x_second(k) for k in range(NCH)]
    core = [send(px[k], pr[k], cs.at[k], cr.at[k], partner) for k in range(NCH)]
    y_a = [(send(sp[k], rp[k], ys.at[k, 0], yr.at[k, 0], yu),
            send(sm[k], rm[k], ys.at[k, 1], yr.at[k, 1], yd)) for k in range(NCH)]
    y_b = [(send(cp[k], qp[k], ys.at[k, 2], yr.at[k, 2], yu),
            send(cm[k], qm[k], ys.at[k, 3], yr.at[k, 3], yd)) for k in range(NCH)]

    swap = [send(fb[k], fr[k], fs.at[k], frs.at[k], across) for k in range(NCH)]

    def start(group):
        for cpy in group:
            cpy.start()

    def arrive(group):
        for cpy in group:
            cpy.wait_recv()

    def dequantize_dy():
        for j in range(32):
            y_, a_, c_, b_ = j // 8, (j // 4) % 2, (j // 2) % 2, j % 2
            val = dv[:, j * 128:(j + 1) * 128].astype(F32) * scales[:, j:j + 1]
            dyp[c_, a_ * 2 + b_, :, y_ * 128:(y_ + 1) * 128] = val.astype(BF16)
        for h in range(2):
            gat[h, x, zrow(z), :] = dyp[h, x]

    def send_dy():
        for h in range(2):
            start(x_dy[h])

    def dequantize_h(k):
        for zz in range(ZN):
            for i in range(WIDTHS[k] // 128):
                col = STARTS[k] + i * 128
                j = ((col // 1024) * 8 + zz) * 8 + (col % 1024) // 128
                val = hv[:, j * 128:(j + 1) * 128].astype(F32) * hs[:, j:j + 1].astype(F32)
                hsend[k][zz, :, i * 128:(i + 1) * 128] = val.astype(BF16)

    def send_h(k):
        if k:
            dequantize_h(k)
        start(z_h[k])
        hz[k][zrow(z), :] = hsend[k][z]

    def ring_dy(h, s):
        arrive(z_dy[h][s - 1] if s else x_dy[h])
        start(z_dy[h][s])

    def requantize_h(k):
        arrive(z_h[k])

        @pl.loop(0, WIDTHS[k] // 128)
        def _(i):
            lanes = pl.ds(pl.multiple_of(i * 128, 128), 128)
            for b in range(LINE // QBLOCK):
                hx[k][xrow(x, b * QBLOCK, QBLOCK), lanes] = requantize(
                    hz[k][b * QBLOCK:(b + 1) * QBLOCK, lanes].astype(F32))

        start(x_h[k])

    def forward_h(k):
        arrive(x_h[k])
        start(x_f[k])

    def requantize_dy(h):
        arrive(z_dy[h][3])
        for b in range(KTOK // 256):

            @pl.loop(0, HALF // 256)
            def _(i):
                at = pl.ds(pl.multiple_of(i * 256, 256), 256)
                vals = [requantize(gat[h, n // 3, (n % 3) * QBLOCK:(n % 3 + 1) * QBLOCK, at].astype(F32))
                        for n in (2 * b, 2 * b + 1)]
                turned = lax.dot_general(eye[...], jnp.concatenate(vals, 0), NT, preferred_element_type=F32)
                gt[pl.ds(pl.multiple_of(h * HALF + i * 256, 256), 256), b * 256:(b + 1) * 256] = turned.astype(BF16)

    def product(h, k):
        if h == first_half[k]:
            arrive(x_f[k])

        @pl.when(c != h)
        def _():
            px[k][...] = jnp.dot(gt[h * HALF:(h + 1) * HALF, :], hx[k][...], preferred_element_type=F32).astype(BF16)
            core[k].start()

        @pl.when(c == h)
        def _():
            po[k][...] = jnp.dot(gt[h * HALF:(h + 1) * HALF, :], hx[k][...], preferred_element_type=F32)

    def part(k, yy, lo):
        return po[k][pl.ds(pl.multiple_of(yy * 128 + lo, 64), 64), :]

    def reduce_first(h, k):
        @pl.when(c == h)
        def _():
            core[k].wait_recv()
            po[k][...] = po[k][...] + pr[k][...].astype(F32)
            sp[k][0] = part(k, y2, 0).astype(BF16)
            sp[k][1] = part(k, y1, 64).astype(BF16)
            sm[k][0] = part(k, y2, 64).astype(BF16)
            sm[k][1] = part(k, y3, 0).astype(BF16)
            start(y_a[k])

    def reduce_second(h, k):
        @pl.when(c == h)
        def _():
            arrive(y_a[k])
            cp[k][...] = (part(k, y1, 0) + rp[k][0].astype(F32)).astype(BF16)
            cm[k][...] = (part(k, y3, 64) + rm[k][0].astype(F32)).astype(BF16)
            start(y_b[k])

    def finish(h, k):
        @pl.when(c == h)
        def _():
            arrive(y_b[k])
            low = (part(k, y, 0) + qp[k][...].astype(F32) + rm[k][1].astype(F32)).astype(BF16)
            high = (part(k, y, 64) + qm[k][...].astype(F32) + rp[k][1].astype(F32)).astype(BF16)

            fb[k][0:64] = low
            fb[k][64:128] = high

            @pl.when(xl == OWNER[k])
            def _():
                put(fb[k], xl, k, 0).start()

            @pl.when(xl != OWNER[k])
            def _():
                swap[k].start()

    def put(src, block, k, n):
        rows = pl.ds(pl.multiple_of(block * 128, 128), 128)
        first = STARTS[k] % 1024
        return pltpu.make_async_copy(src, out.at[rows, first:first + WIDTHS[k]], os.at[k, n])

    def conclude():
        for group in x_dy + z_h + z_dy[0] + z_dy[1] + x_h + x_f:
            for cpy in group:
                cpy.wait_send()
        for k in range(NCH):
            for cpy in (core[k],) + y_a[k] + y_b[k]:
                cpy.wait_send()
        for k in last_chunks:
            @pl.when(xl == OWNER[k])
            def _():
                swap[k].wait_recv()
                put(fr[k], 1 - xl, k, 1).start()

            @pl.when(xl != OWNER[k])
            def _():
                swap[k].wait_send()
        for k in last_chunks:
            @pl.when(xl == OWNER[k])
            def _():
                put(fb[k], xl, k, 0).wait()
                put(fr[k], 1 - xl, k, 1).wait()

    scales = lax.dot_general(eye[0:TOK, 0:TOK], ds[...], NT, preferred_element_type=F32)
    first_half, last_chunks = {}, []
    for step in ORDER:
        if step[0] == "P":
            first_half.setdefault(step[2], step[1])
        if step[0] == "E":
            last_chunks = [k for k in last_chunks if k != step[2]] + [step[2]]
    steps = dict(dy=dequantize_dy, bar=lambda: pl.semaphore_wait(barrier, len(peers)), x0=send_dy, h=send_h,
                 s=ring_dy, r=requantize_h, f=forward_h, q=requantize_dy, P=product, A=reduce_first,
                 B=reduce_second, E=finish, END=conclude)
    dequantize_h(0)
    for step in ORDER:
        steps[step[0]](*step[1:])


def shards(h_values, h_scales, dy_values, dy_scales):
    dma = pltpu.SemaphoreType.DMA
    anywhere = pl.BlockSpec(memory_space=pl.ANY)

    def chunks(shape, dtype=BF16):
        return [pltpu.VMEM(shape + (width,), dtype) for width in WIDTHS]

    return pl.pallas_call(
        kernel,
        out_shape=jax.ShapeDtypeStruct((256, 1024), BF16),
        in_specs=[anywhere] * 4,
        out_specs=anywhere,
        scratch_shapes=[
            pltpu.VMEM((TOK, 16384), BF16),
            pltpu.VMEM((TOK, 128), BF16),
            pltpu.VMEM((TOK, 4096), BF16),
            pltpu.VMEM((32, TOK), BF16),
            pltpu.VMEM((256, 256), BF16),
            pltpu.VMEM((2, XN, TOK, HALF), BF16),
            pltpu.VMEM((2, XN, LINE, HALF), BF16),
            chunks((ZN, TOK)),
            chunks((LINE,)),
            chunks((KTOK,)),
            pltpu.VMEM((2 * HALF, KTOK), BF16),
            chunks((HALF,)),
            chunks((HALF,)),
            chunks((HALF,), F32),
            chunks((2, 64)), chunks((2, 64)), chunks((2, 64)), chunks((2, 64)),
            chunks((64,)), chunks((64,)), chunks((64,)), chunks((64,)),
            chunks((128,)), chunks((128,)),
            dma((4,)),
            dma((NCH, 7)), dma((NCH, 7)),
            dma((2, 3)), dma((2, 3)),
            dma((2, 2, 4)), dma((2, 2, 4)),
            dma((NCH, 2)), dma((NCH, 2)),
            dma((NCH, 2)), dma((NCH, 2)),
            dma((NCH,)), dma((NCH,)),
            dma((NCH, 4)), dma((NCH, 4)),
            dma((NCH,)), dma((NCH,)),
            dma((NCH, 2)),
        ],
        compiler_params=pltpu.CompilerParams(
            collective_id=0, has_side_effects=True, vmem_limit_bytes=60 * 1024 * 1024),
    )(h_values, h_scales, dy_values, dy_scales.T)


def solution(mesh):
    placed = P(("dp", "tensor"), None)
    return jax.shard_map(
        shards, mesh=mesh, in_specs=(placed,) * 4, out_specs=P("dp", "tensor"), check_vma=False)
```

```python
import jax
import jax.numpy as jnp
from jax import lax
from jax.experimental import pallas as pl
from jax.experimental.pallas import tpu as pltpu
from jax.sharding import PartitionSpec as P

QBLOCK = 128
MESH = pl.DeviceIdType.MESH
XN, YN, ZN = 4, 4, 8
TOK = 48
LINE = ZN * TOK
KTOK = XN * LINE
HALF = 512
COLS = 2048
WIDTHS = (128, 384, 512, 512, 256, 128, 128)
NCH = len(WIDTHS)
STARTS = tuple(sum(WIDTHS[:k]) for k in range(NCH))
OWNER = tuple(start // 1024 for start in STARTS)
F32, BF16 = jnp.float32, jnp.bfloat16
NT = (((1,), (1,)), ((), ()))
ORDER = (
    ("dy",), ("bar",), ("x0",), ("h", 0), ("h", 2), ("s", 0, 0), ("h", 1), ("h", 3), ("r", 2), ("r", 0), ("f", 2),
    ("f", 0), ("r", 1), ("s", 0, 1), ("s", 1, 0), ("r", 3), ("s", 0, 2), ("f", 1), ("s", 1, 1), ("s", 0, 3),
    ("s", 1, 2), ("h", 4), ("f", 3), ("q", 0), ("P", 0, 2), ("P", 0, 1), ("P", 0, 3), ("s", 1, 3), ("A", 0, 2),
    ("A", 0, 1), ("h", 6), ("P", 0, 0), ("h", 5), ("r", 4), ("A", 0, 0), ("B", 0, 2), ("A", 0, 3), ("q", 1),
    ("B", 0, 1), ("r", 6), ("P", 1, 0), ("P", 1, 3), ("f", 4), ("B", 0, 3), ("P", 1, 2), ("r", 5), ("A", 1, 0),
    ("A", 1, 3), ("P", 1, 1), ("f", 6), ("A", 1, 2), ("P", 1, 4), ("P", 0, 4), ("A", 1, 1), ("f", 5), ("B", 1, 3),
    ("A", 1, 4), ("B", 0, 0), ("B", 1, 2), ("P", 1, 6), ("P", 0, 6), ("A", 0, 4), ("B", 1, 1), ("P", 1, 5),
    ("P", 0, 5), ("E", 0, 3), ("A", 1, 6), ("A", 0, 6), ("B", 1, 0), ("E", 0, 1), ("A", 1, 5), ("E", 0, 2),
    ("A", 0, 5), ("B", 1, 4), ("E", 1, 3), ("B", 0, 4), ("E", 1, 1), ("E", 1, 2), ("B", 1, 6), ("E", 1, 0),
    ("B", 0, 6), ("B", 1, 5), ("B", 0, 5), ("E", 1, 4), ("E", 0, 0), ("E", 1, 6), ("E", 0, 4), ("E", 0, 6),
    ("E", 1, 5), ("E", 0, 5), ("END",),
)


def requantize(block):
    largest = jnp.max(jnp.abs(block), axis=0, keepdims=True)
    scale = ((largest + 1e-6) / 448.0).astype(BF16).astype(F32)
    quantized = (block * (1.0 / scale)).astype(BF16).astype(F32)
    return (quantized * scale).astype(BF16)


def kernel(hv_hbm, hs_hbm, dv_hbm, ds_hbm, out,
           hv, hs, dv, ds, eye, dyp, gat, hsend, hz, hx, gt, px, pr, po,
           sp, sm, rp, rm, cp, cm, qp, qm, fb, fr,
           ld, hss, hrs, dxs, dxr, dzs, dzr, xss, xrs, xfs, xfr, cs, cr, ys, yr, fs, frs, os):
    dp, t = lax.axis_index("dp"), lax.axis_index("tensor")
    c, xh, y = dp % 2, (dp // 2) % 2, dp // 4
    xl, z = t // 8, t % 8
    x = xh * 2 + xl

    def dev(x_=None, y_=None, z_=None, c_=None):
        x_ = x if x_ is None else x_
        y_ = y if y_ is None else y_
        z_ = z if z_ is None else z_
        c_ = c if c_ is None else c_
        return ((y_ * 2 + x_ // 2) * 2 + c_, (x_ % 2) * 8 + z_)

    def send(src, dst, ssem, rsem, to):
        return pltpu.make_async_remote_copy(
            src_ref=src, dst_ref=dst, send_sem=ssem, recv_sem=rsem, device_id=to, device_id_type=MESH)

    def zrow(zs):
        return pl.ds(pl.multiple_of(zs * TOK, 16), TOK)

    def xrow(xs, lo=0, n=LINE):
        return pl.ds(pl.multiple_of(xs * LINE + lo, 16), n)

    barrier = pltpu.get_barrier_semaphore()
    peers = ([dev(x_=(x + d) % XN) for d in range(1, XN)] + [dev(y_=(y + d) % YN) for d in (1, 3)]
             + [dev(z_=(z + d) % ZN) for d in range(1, ZN)] + [dev(c_=1 - c)])
    for peer in peers:
        pl.semaphore_signal(barrier, inc=1, device_id=peer, device_id_type=MESH)

    loads = [pltpu.make_async_copy(a, b, ld.at[n])
             for n, (a, b) in enumerate(((hv_hbm, hv), (hs_hbm, hs), (dv_hbm, dv), (ds_hbm, ds)))]
    for cpy in loads:
        cpy.start()
    eye[...] = (lax.broadcasted_iota(jnp.int32, (256, 256), 0)
                == lax.broadcasted_iota(jnp.int32, (256, 256), 1)).astype(F32).astype(BF16)
    for cpy in loads:
        cpy.wait()

    zu, zd = dev(z_=(z + 1) % ZN), dev(z_=(z + 7) % ZN)
    xu, xd = dev(x_=(x + 1) % XN), dev(x_=(x + 3) % XN)
    yu, yd = dev(y_=(y + 1) % YN), dev(y_=(y + 3) % YN)
    partner, across = dev(c_=1 - c), dev(x_=xh * 2 + 1 - xl)
    xup, xdn = (x + 3) % XN, (x + 1) % XN
    y1, y2, y3 = (y + 1) % YN, (y + 2) % YN, (y + 3) % YN

    x_dy = [[send(dyp.at[h, (x + d) % XN], gat.at[h, x, zrow(z)], dxs.at[h, d - 1], dxr.at[h, d - 1],
                  dev(x_=(x + d) % XN)) for d in range(1, XN)] for h in range(2)]
    z_h = [[send(hsend[k].at[(z + d) % ZN], hz[k].at[zrow(z)], hss.at[k, n], hrs.at[k, n], dev(z_=(z + d) % ZN))
            for n, d in enumerate((1, 7, 2, 6, 3, 5, 4))] for k in range(NCH)]

    def ring(h, s):
        lo, hi = (slice(0, 2), slice(2, 4)) if s == 3 else (slice(None), slice(None))
        up, dn = gat.at[h, lo, zrow((z + 8 - s) % ZN)], gat.at[h, hi, zrow((z + s) % ZN)]
        return (send(up, up, dzs.at[h, 0, s], dzr.at[h, 0, s], zu), send(dn, dn, dzs.at[h, 1, s], dzr.at[h, 1, s], zd))

    z_dy = [[ring(h, s) for s in range(4)] for h in range(2)]

    def x_first(k):
        mine = hx[k].at[xrow(x)]
        return (send(mine, mine, xss.at[k, 0], xrs.at[k, 0], xu), send(mine, mine, xss.at[k, 1], xrs.at[k, 1], xd))

    def x_second(k):
        up, dn = hx[k].at[xrow(xup, 0, LINE // 2)], hx[k].at[xrow(xdn, LINE // 2, LINE // 2)]
        return (send(up, up, xfs.at[k, 0], xfr.at[k, 0], xu), send(dn, dn, xfs.at[k, 1], xfr.at[k, 1], xd))

    x_h = [x_first(k) for k in range(NCH)]
    x_f = [x_second(k) for k in range(NCH)]
    core = [send(px[k], pr[k], cs.at[k], cr.at[k], partner) for k in range(NCH)]
    y_a = [(send(sp[k], rp[k], ys.at[k, 0], yr.at[k, 0], yu),
            send(sm[k], rm[k], ys.at[k, 1], yr.at[k, 1], yd)) for k in range(NCH)]
    y_b = [(send(cp[k], qp[k], ys.at[k, 2], yr.at[k, 2], yu),
            send(cm[k], qm[k], ys.at[k, 3], yr.at[k, 3], yd)) for k in range(NCH)]

    swap = [send(fb[k], fr[k], fs.at[k], frs.at[k], across) for k in range(NCH)]

    def start(group):
        for cpy in group:
            cpy.start()

    def arrive(group):
        for cpy in group:
            cpy.wait_recv()

    def dequantize_dy():
        for j in range(32):
            y_, a_, c_, b_ = j // 8, (j // 4) % 2, (j // 2) % 2, j % 2
            val = dv[:, j * 128:(j + 1) * 128].astype(F32) * scales[:, j:j + 1]
            dyp[c_, a_ * 2 + b_, :, y_ * 128:(y_ + 1) * 128] = val.astype(BF16)
        for h in range(2):
            gat[h, x, zrow(z), :] = dyp[h, x]

    def send_dy():
        for h in range(2):
            start(x_dy[h])

    def dequantize_h(k):
        for zz in range(ZN):
            for i in range(WIDTHS[k] // 128):
                col = STARTS[k] + i * 128
                j = ((col // 1024) * 8 + zz) * 8 + (col % 1024) // 128
                val = hv[:, j * 128:(j + 1) * 128].astype(F32) * hs[:, j:j + 1].astype(F32)
                hsend[k][zz, :, i * 128:(i + 1) * 128] = val.astype(BF16)

    def send_h(k):
        if k:
            dequantize_h(k)
        start(z_h[k])
        hz[k][zrow(z), :] = hsend[k][z]

    def ring_dy(h, s):
        arrive(z_dy[h][s - 1] if s else x_dy[h])
        start(z_dy[h][s])

    def requantize_h(k):
        arrive(z_h[k])

        @pl.loop(0, WIDTHS[k] // 128)
        def _(i):
            lanes = pl.ds(pl.multiple_of(i * 128, 128), 128)
            for b in range(LINE // QBLOCK):
                hx[k][xrow(x, b * QBLOCK, QBLOCK), lanes] = requantize(
                    hz[k][b * QBLOCK:(b + 1) * QBLOCK, lanes].astype(F32))

        start(x_h[k])

    def forward_h(k):
        arrive(x_h[k])
        start(x_f[k])

    def requantize_dy(h):
        arrive(z_dy[h][3])
        for b in range(KTOK // 256):

            @pl.loop(0, HALF // 256)
            def _(i):
                at = pl.ds(pl.multiple_of(i * 256, 256), 256)
                vals = [requantize(gat[h, n // 3, (n % 3) * QBLOCK:(n % 3 + 1) * QBLOCK, at].astype(F32))
                        for n in (2 * b, 2 * b + 1)]
                turned = lax.dot_general(eye[...], jnp.concatenate(vals, 0), NT, preferred_element_type=F32)
                gt[pl.ds(pl.multiple_of(h * HALF + i * 256, 256), 256), b * 256:(b + 1) * 256] = turned.astype(BF16)

    def product(h, k):
        if h == first_half[k]:
            arrive(x_f[k])

        @pl.when(c != h)
        def _():
            px[k][...] = jnp.dot(gt[h * HALF:(h + 1) * HALF, :], hx[k][...], preferred_element_type=F32).astype(BF16)
            core[k].start()

        @pl.when(c == h)
        def _():
            po[k][...] = jnp.dot(gt[h * HALF:(h + 1) * HALF, :], hx[k][...], preferred_element_type=F32)

    def part(k, yy, lo):
        return po[k][pl.ds(pl.multiple_of(yy * 128 + lo, 64), 64), :]

    def reduce_first(h, k):
        @pl.when(c == h)
        def _():
            core[k].wait_recv()
            po[k][...] = po[k][...] + pr[k][...].astype(F32)
            sp[k][0] = part(k, y2, 0).astype(BF16)
            sp[k][1] = part(k, y1, 64).astype(BF16)
            sm[k][0] = part(k, y2, 64).astype(BF16)
            sm[k][1] = part(k, y3, 0).astype(BF16)
            start(y_a[k])

    def reduce_second(h, k):
        @pl.when(c == h)
        def _():
            arrive(y_a[k])
            cp[k][...] = (part(k, y1, 0) + rp[k][0].astype(F32)).astype(BF16)
            cm[k][...] = (part(k, y3, 64) + rm[k][0].astype(F32)).astype(BF16)
            start(y_b[k])

    def finish(h, k):
        @pl.when(c == h)
        def _():
            arrive(y_b[k])
            low = (part(k, y, 0) + qp[k][...].astype(F32) + rm[k][1].astype(F32)).astype(BF16)
            high = (part(k, y, 64) + qm[k][...].astype(F32) + rp[k][1].astype(F32)).astype(BF16)

            fb[k][0:64] = low
            fb[k][64:128] = high

            @pl.when(xl == OWNER[k])
            def _():
                put(fb[k], xl, k, 0).start()

            @pl.when(xl != OWNER[k])
            def _():
                swap[k].start()

    def put(src, block, k, n):
        rows = pl.ds(pl.multiple_of(block * 128, 128), 128)
        first = STARTS[k] % 1024
        return pltpu.make_async_copy(src, out.at[rows, first:first + WIDTHS[k]], os.at[k, n])

    def conclude():
        for group in x_dy + z_h + z_dy[0] + z_dy[1] + x_h + x_f:
            for cpy in group:
                cpy.wait_send()
        for k in range(NCH):
            for cpy in (core[k],) + y_a[k] + y_b[k]:
                cpy.wait_send()
        for k in last_chunks:
            @pl.when(xl == OWNER[k])
            def _():
                swap[k].wait_recv()
                put(fr[k], 1 - xl, k, 1).start()

            @pl.when(xl != OWNER[k])
            def _():
                swap[k].wait_send()
        for k in last_chunks:
            @pl.when(xl == OWNER[k])
            def _():
                put(fb[k], xl, k, 0).wait()
                put(fr[k], 1 - xl, k, 1).wait()

    scales = lax.dot_general(eye[0:TOK, 0:TOK], ds[...], NT, preferred_element_type=F32)
    first_half, last_chunks = {}, []
    for step in ORDER:
        if step[0] == "P":
            first_half.setdefault(step[2], step[1])
        if step[0] == "E":
            last_chunks = [k for k in last_chunks if k != step[2]] + [step[2]]
    steps = dict(dy=dequantize_dy, bar=lambda: pl.semaphore_wait(barrier, len(peers)), x0=send_dy, h=send_h,
                 s=ring_dy, r=requantize_h, f=forward_h, q=requantize_dy, P=product, A=reduce_first,
                 B=reduce_second, E=finish, END=conclude)
    dequantize_h(0)
    for step in ORDER:
        steps[step[0]](*step[1:])


def shards(h_values, h_scales, dy_values, dy_scales):
    dma = pltpu.SemaphoreType.DMA
    anywhere = pl.BlockSpec(memory_space=pl.ANY)

    def chunks(shape, dtype=BF16):
        return [pltpu.VMEM(shape + (width,), dtype) for width in WIDTHS]

    return pl.pallas_call(
        kernel,
        out_shape=jax.ShapeDtypeStruct((256, 1024), BF16),
        in_specs=[anywhere] * 4,
        out_specs=anywhere,
        scratch_shapes=[
            pltpu.VMEM((TOK, 16384), BF16),
            pltpu.VMEM((TOK, 128), BF16),
            pltpu.VMEM((TOK, 4096), BF16),
            pltpu.VMEM((32, TOK), BF16),
            pltpu.VMEM((256, 256), BF16),
            pltpu.VMEM((2, XN, TOK, HALF), BF16),
            pltpu.VMEM((2, XN, LINE, HALF), BF16),
            chunks((ZN, TOK)),
            chunks((LINE,)),
            chunks((KTOK,)),
            pltpu.VMEM((2 * HALF, KTOK), BF16),
            chunks((HALF,)),
            chunks((HALF,)),
            chunks((HALF,), F32),
            chunks((2, 64)), chunks((2, 64)), chunks((2, 64)), chunks((2, 64)),
            chunks((64,)), chunks((64,)), chunks((64,)), chunks((64,)),
            chunks((128,)), chunks((128,)),
            dma((4,)),
            dma((NCH, 7)), dma((NCH, 7)),
            dma((2, 3)), dma((2, 3)),
            dma((2, 2, 4)), dma((2, 2, 4)),
            dma((NCH, 2)), dma((NCH, 2)),
            dma((NCH, 2)), dma((NCH, 2)),
            dma((NCH,)), dma((NCH,)),
            dma((NCH, 4)), dma((NCH, 4)),
            dma((NCH,)), dma((NCH,)),
            dma((NCH, 2)),
        ],
        compiler_params=pltpu.CompilerParams(
            collective_id=0, has_side_effects=True, vmem_limit_bytes=60 * 1024 * 1024),
    )(h_values, h_scales, dy_values, dy_scales.T)


def solution(mesh):
    placed = P(("dp", "tensor"), None)
    return jax.shard_map(
        shards, mesh=mesh, in_specs=(placed,) * 4, out_specs=P("dp", "tensor"), check_vma=False)
```
